32 devices in a mesh: row: 4 (over z), col: 4 (over x, core), depth: 2 (over y).
Axes of the slice: x: 2, y: 2, z: 4, core: 2. Of those that a mesh axis runs over, the one named last changes fastest.
Arguments:
- heads_concat: bfloat16 [2048, 16384], P('row', ('depth', 'col')), may hold values from -6 to 6
- w_out: bfloat16 [16384, 7168], P(('depth', 'row'), 'col'), may hold values from -0.046875 to 0.046875
Outputs:
- projected: bfloat16 [2048, 7168], P('row', ('col', 'depth'))
The draws below stay inside these ranges and needn't reach their ends.
All inputs are finite; a program needn't handle non-finite values.
Results may differ from the reference program's by a relative error of at most 0.001.
Values may be sent and summed in bfloat16 or wider, within the bound.
No kernel may reach another device: no remote copies, remote signals or barrier semaphores. Data moves between devices by JAX's collectives and lax.ppermute only.
A program may use at most 128 MiB of HBM per device.

```python
import jax
import jax.numpy as jnp

D = 7168
K = 16384
TOKENS = 2048


def block_levels(stream_key, dims, cuts, least, top_value):
    factor_of, own = 1.0, jax.random.fold_in(stream_key, 6)
    for dim, parts in cuts:
        draws = jnp.exp(jax.random.uniform(jax.random.fold_in(own, dim), (parts,), jnp.float32, least / len(cuts), top_value / len(cuts)))
        factor_of = factor_of * jnp.repeat(draws, dims[dim] // parts).reshape([-1 if axis == dim else 1 for axis in range(len(dims))])
    return factor_of


def bell_draw(stream_key, extent, scale, limit, pieces=(), held_as=jnp.bfloat16):
    values = scale * jax.random.normal(stream_key, extent, jnp.float32)
    if pieces:
        values = values * block_levels(stream_key, extent, pieces, -0.22, 0.18)
    return jnp.clip(values, -limit, limit).astype(held_as)


def setup_inputs(seed: int = 0) -> dict:
    key_of = jax.random.split(jax.random.key(seed), 3)
    return {
        "heads_concat": bell_draw(key_of[0], (TOKENS, K), 1.0, 6.0, ((0, 4), (1, 8))),
        "w_out": bell_draw(key_of[1], (K, D), K ** -0.5, 0.046875, ((0, 8), (1, 4))),
    }


def reference(heads_concat, w_out):
    product = jnp.dot(heads_concat, w_out, preferred_element_type=jnp.float32)
    return product.astype(jnp.bfloat16)
```

```python
import jax
import jax.numpy as jnp
from jax import lax
from jax.sharding import PartitionSpec as P


def solution(mesh):
    rows, cols, depths = mesh.shape["row"], mesh.shape["col"], mesh.shape["depth"]
    per_col = rows // cols

    def at(row, col):
        return row * cols + col

    def per_device(heads, weights):
        row, depth = lax.axis_index("row"), lax.axis_index("depth")
        width = weights.shape[1] // depths
        feats = weights.shape[0]

        def columns(of):
            return lax.dynamic_slice_in_dim(weights, of * width, width, 1)

        mine = [columns(depth)]
        for shift in range(1, depths):
            ring = [(d, (d + shift) % depths) for d in range(depths)]
            mine.append(lax.ppermute(columns((depth + shift) % depths), "depth", ring))

        moved = []
        for turn in range(per_col):
            piece = (turn + row // cols) % per_col
            pairs = []
            for t in range(rows):
                for k in range(cols):
                    pairs.append((at(t, k), at(k * per_col + (turn + t // cols) % per_col, t % cols)))
            block = lax.dynamic_slice_in_dim(heads, piece * feats, feats, 1)
            moved.append(lax.ppermute(block, ("row", "col"), pairs))
        turns = [lax.all_gather(block, ("col", "depth")) for block in moved]

        gathered = jnp.stack(turns).reshape((per_col, cols, depths) + moved[0].shape)
        if per_col > 1:
            order = (row % per_col - jnp.arange(per_col)) % per_col
            gathered = jnp.take(gathered, order, axis=0)
        total = None
        for shift in range(depths):
            part = lax.dynamic_index_in_dim(gathered, (depth - shift) % depths, 2, keepdims=False)
            part = part.reshape((-1, feats))
            term = jnp.dot(part, mine[shift], preferred_element_type=jnp.float32)
            total = term if total is None else total + term
        summed = lax.psum_scatter(total, "row", scatter_dimension=0, tiled=True)
        return summed.astype(jnp.bfloat16)

    return jax.shard_map(
        per_device,
        mesh=mesh,
        in_specs=(P("row", ("depth", "col")), P(("depth", "row"), "col")),
        out_specs=P("row", ("col", "depth")),
        check_vma=False,
    )
```
